1024 devices in a mesh: dp: 32 (over y, x, core), expert: 32 (over z).
Axes of the slice: x: 4, y: 4, z: 32, core: 2. Of those that a mesh axis runs over, the one named last changes fastest.
Arguments:
- tokens: bfloat16 [131072, 2048], P(('dp', 'expert')), may hold values from -6 to 6
- out_grad: bfloat16 [131072, 2048], P(('dp', 'expert')), may hold values from -6 to 6
- gate_prob: float32 [131072, 1], P(('dp', 'expert')), may hold values from 0.2 to 1
- routing: int32 [131072, 1], P(('dp', 'expert')), may hold values from 0 to 31; in each aligned block of 128 rows (0 to 127, 128 to 255, ...) at most 8 rows name the same one
- expert_weights: bfloat16 [32, 2048, 1152], P('expert'), may hold values from -0.125 to 0.125
Outputs:
- input_grad: bfloat16 [131072, 2048], P(('dp', 'expert'))
- weight_grad: float32 [32, 2048, 1152], P('expert', 'dp')
The draws below stay inside these ranges and needn't reach their ends.
Inputs may be any that keep to these rules, and one draw needn't show every extreme that they name: `routing`: among the tokens of one device at most 8 go to any one expert; in some devices' tokens an expert gets exactly 8.
All inputs are finite; a program needn't handle non-finite values.
Results may differ from the reference program's by a relative error of at most 0.014.
Values may be sent and summed in bfloat16 or wider, within the bound.
A program may use at most 64 MiB of HBM per device.

```python
import math
from functools import partial
import jax
import jax.numpy as jnp
import numpy as np
from jax import lax

D = 2048
FF = 384
TOK_DEV = 128
TOKENS = 131072
EXPERTS_TURN = 32
CAP = 8
GROUP_ROWS = 4096
N_DP = 32
N_EXPERT = 32


def block_levels(key, shape, shards, smallest, high):
    level, own = 1.0, jax.random.fold_in(key, 6)
    for axis_at, shards_of in shards:
        heights = jnp.exp(jax.random.uniform(jax.random.fold_in(own, axis_at), (shards_of,), jnp.float32, smallest / len(shards), high / len(shards)))
        level = level * jnp.repeat(heights, shape[axis_at] // shards_of).reshape([-1 if axis == axis_at else 1 for axis in range(len(shape))])
    return level


def shared_out(stream_key, own, number, rows, number_of, top, most, slope):
    order = jax.random.permutation(stream_key, number_of)
    heavy_load, common = shares(number_of, rows * top, most, slope, True), shares(number_of, rows * top, most, slope, False)
    places = jnp.arange(number_of)

    def named(sizes, rotation):
        used = int((sizes > 0).sum())
        fixed = max(1, used // 4)
        moved = fixed + (places - fixed + rotation * (used - fixed)) % max(1, number_of - fixed)
        return jnp.zeros((number_of,), jnp.int32).at[order[jnp.where(places < fixed, places, moved)]].set(jnp.asarray(sizes, jnp.int32))

    sizes = jnp.where(number % 4 == 0, named(heavy_load, number // 4), named(common, number - number // 4 - 1))
    mixed = jax.random.permutation(jax.random.fold_in(own, 3), number_of)
    giver, receiver = mixed[0:number_of // 2 * 2:2], mixed[1:number_of // 2 * 2:2]
    slack = jnp.minimum(sizes[giver] - 1, most - sizes[receiver]) // 2
    slack = jnp.where((giver == order[0]) | (receiver == order[0]) | (sizes[receiver] == 0), 0, jnp.maximum(slack, 0))
    moved = jax.random.randint(jax.random.fold_in(own, 4), (number_of // 2,), 0, 1 << 20) % (slack + 1)
    sizes = sizes.at[giver].add(-moved).at[receiver].add(moved)
    labels = jnp.searchsorted(jnp.cumsum(sizes), jnp.arange(rows * top), side="right").astype(jnp.int32)
    grid = labels.reshape(top, rows).T
    grid = grid[jax.random.permutation(jax.random.fold_in(own, 1), rows)]
    rotation = jax.random.randint(jax.random.fold_in(own, 2), (rows, 1), 0, top)
    return jnp.take_along_axis(grid, (jnp.arange(top)[None, :] + rotation) % top, axis=1)


def shares(number_of, total, reach, slope, full):
    loads = [(1 << 20) // math.isqrt(standing ** slope) + 1 for standing in range(1, number_of + 1)]
    largest = reach if full else min(reach, max(-(-total // number_of), total * loads[0] // sum(loads)))
    least = 1 if total - largest >= number_of - 1 else 0
    counts, rest = [largest] + [least] * (number_of - 1), total - largest - least * (number_of - 1)
    while rest > 0:
        candidates = [i for i in range(1, number_of) if counts[i] < largest] or [i for i in range(1, number_of) if counts[i] < reach]
        whole, left = sum([loads[i] for i in candidates]), rest
        for i in candidates:
            more = min(reach - counts[i], max(1, left * loads[i] // whole), rest)
            counts[i] = counts[i] + more
            rest = rest - more
    return np.array(counts)


def noise(rng, extent, width, reach, pieces=(), kind=jnp.bfloat16):
    drawn = jax.random.normal(rng, extent, jnp.float32) * width
    if len(pieces) > 0:
        drawn = block_levels(rng, extent, pieces, -0.22, 0.18) * drawn
    return jnp.clip(drawn, min=-reach, max=reach).astype(kind)


def setup_inputs(seed: int = 0) -> dict:
    streams_of = jax.random.split(jax.random.key(seed), 6)
    tokens = noise(streams_of[0], (TOKENS, D), 1.0, 6.0, ((0, 1024),))
    out_grad = noise(streams_of[1], (TOKENS, D), 1.0, 6.0, ((0, 1024),))
    gate_prob = jnp.clip(0.2 + 0.8 * jax.random.uniform(streams_of[2], (TOKENS, 1), jnp.float32) ** block_levels(streams_of[2], (TOKENS, 1), ((0, 1024),), -0.2, 0.2), 0.2, 1.0)
    routing_keys = jax.random.split(jax.random.fold_in(streams_of[3], 1), TOKENS // TOK_DEV)
    routing_turns = jax.random.permutation(jax.random.fold_in(streams_of[3], 3), TOKENS // TOK_DEV)
    routing = jax.vmap(lambda own, number: shared_out(jax.random.fold_in(streams_of[3], 2), own, number, TOK_DEV, N_EXPERT, 1, CAP, 2))(routing_keys, routing_turns).reshape((TOKENS, 1))
    expert_weights = noise(streams_of[4], (EXPERTS_TURN, D, 3 * FF), D ** -0.5, 0.125, ((0, 32),))
    return {"tokens": tokens, "out_grad": out_grad, "gate_prob": gate_prob, "routing": routing, "expert_weights": expert_weights}


def slot_of(route_block, capacity, experts):
    onehot = (route_block[:, None] == jnp.arange(experts, dtype=jnp.int32)[None, :]).astype(jnp.int32)
    before = jnp.cumsum(onehot, axis=0) - onehot
    position = jnp.sum(before * onehot, axis=1).astype(jnp.int32)
    return (route_block * capacity + position).astype(jnp.int32)


def expert_rows(weights, rows_in, grad_in):
    hidden_width = weights.shape[1] // 3
    pair_weights = weights[:, :2 * hidden_width]
    down_weights = weights[:, 2 * hidden_width:]
    pre_act = jnp.dot(rows_in, pair_weights, preferred_element_type=jnp.float32)
    pre_gate = pre_act[:, :hidden_width]
    pre_up = pre_act[:, hidden_width:]
    sigmoid_gate = jax.nn.sigmoid(pre_gate)
    active = pre_gate * sigmoid_gate
    hidden = (active * pre_up).astype(jnp.bfloat16)
    grad_hidden = jnp.dot(grad_in, down_weights, preferred_element_type=jnp.float32)
    grad_gate = grad_hidden * pre_up * (sigmoid_gate * (1.0 + pre_gate * (1.0 - sigmoid_gate)))
    grad_up = grad_hidden * active
    grad_pair = jnp.concatenate([grad_gate.astype(jnp.bfloat16), grad_up.astype(jnp.bfloat16)], axis=1)
    returned = lax.dot_general(grad_pair, pair_weights, (((1,), (1,)), ((), ())), preferred_element_type=jnp.float32)
    return returned.astype(jnp.bfloat16), hidden, grad_pair


def weight_term(rows_in, grad_in, hidden, grad_pair, grad_scale):
    contract = (((0,), (0,)), ((), ()))
    first_part = lax.dot_general(rows_in, grad_pair, contract, preferred_element_type=jnp.float32)
    second = lax.dot_general(grad_in, hidden, contract, preferred_element_type=jnp.float32)
    return grad_scale * jnp.concatenate([first_part, second], axis=1)


def reference(tokens, out_grad, gate_prob, routing, expert_weights):
    model_width = tokens.shape[1]
    grad_scale = float(GROUP_ROWS) ** -0.5
    scaled = (gate_prob * out_grad.astype(jnp.float32)).astype(jnp.bfloat16)
    tok_x = tokens.reshape(N_DP, N_EXPERT, TOK_DEV, model_width)
    tok_g = scaled.reshape(N_DP, N_EXPERT, TOK_DEV, model_width)
    routes = routing.reshape(N_DP, N_EXPERT, TOK_DEV)
    slotter = jax.vmap(partial(slot_of, capacity=CAP, experts=N_EXPERT))

    def one_expert(operands):
        weights, rows_in, grad_in = operands
        returned, hidden, grad_pair = expert_rows(weights, rows_in, grad_in)
        rounded = weight_term(rows_in, grad_in, hidden, grad_pair, grad_scale).astype(jnp.bfloat16)
        rounded = lax.optimization_barrier(rounded)
        return returned, rounded.astype(jnp.float32)

    def replica(running, blocks):
        block_x, block_g, block_r = blocks
        slot_index = slotter(block_r)
        source = jnp.broadcast_to(jnp.arange(N_EXPERT, dtype=jnp.int32)[:, None], slot_index.shape)
        buf_x = jnp.zeros((N_EXPERT, N_EXPERT * CAP, model_width), jnp.bfloat16).at[source, slot_index].set(block_x)
        buf_g = jnp.zeros((N_EXPERT, N_EXPERT * CAP, model_width), jnp.bfloat16).at[source, slot_index].set(block_g)
        buf_x = buf_x.reshape(N_EXPERT, N_EXPERT, CAP, model_width).transpose(1, 0, 2, 3).reshape(N_EXPERT, N_EXPERT * CAP, model_width)
        buf_g = buf_g.reshape(N_EXPERT, N_EXPERT, CAP, model_width).transpose(1, 0, 2, 3).reshape(N_EXPERT, N_EXPERT * CAP, model_width)
        returned, terms = lax.map(one_expert, (expert_weights, buf_x, buf_g))
        returned = returned.reshape(N_EXPERT, N_EXPERT, CAP, model_width).transpose(1, 0, 2, 3).reshape(N_EXPERT, N_EXPERT * CAP, model_width)
        return running + terms, returned[source, slot_index]

    initial = jnp.zeros((N_EXPERT, model_width, expert_weights.shape[2]), jnp.float32)
    totals, input_grads = lax.scan(replica, initial, (tok_x, tok_g, routes))
    return input_grads.reshape(TOKENS, model_width), totals
```

```python
import jax
import jax.numpy as jnp
from jax import lax
from jax.sharding import Mesh
from jax.sharding import PartitionSpec as P

DP = ("dp_0", "dp_1", "dp_2")
DP_EXPERT = ("dp_0", "dp_1", "dp_2", "expert")


def side_by_side(arrays, axis, split_dim, concat_dim, along):
    widths = [a.shape[along] for a in arrays]
    both = jnp.concatenate(arrays, axis=along)
    filled = lax.all_to_all(both, axis, split_axis=split_dim, concat_axis=concat_dim, tiled=True)
    return tuple(jnp.split(filled, [sum(widths[:k]) for k in range(1, len(widths))], axis=along))


def slot_of(route_block, capacity, experts):
    onehot = (route_block[:, None] == jnp.arange(experts, dtype=jnp.int32)[None, :]).astype(
        jnp.int32
    )
    before = jnp.cumsum(onehot, axis=0) - onehot
    position = jnp.sum(before * onehot, axis=1)
    return route_block * capacity + position


def expert_rows(weights, rows_in, grad_in):
    hidden_width = weights.shape[1] // 3
    pair_weights = weights[:, : 2 * hidden_width]
    down_weights = weights[:, 2 * hidden_width :]
    pre_act = jnp.dot(rows_in, pair_weights, preferred_element_type=jnp.float32)
    pre_gate = pre_act[:, :hidden_width]
    pre_up = pre_act[:, hidden_width:]
    sigmoid_gate = jax.nn.sigmoid(pre_gate)
    active = pre_gate * sigmoid_gate
    hidden = (active * pre_up).astype(jnp.bfloat16)
    grad_hidden = jnp.dot(grad_in, down_weights, preferred_element_type=jnp.float32)
    grad_gate = grad_hidden * pre_up * (sigmoid_gate * (1.0 + pre_gate * (1.0 - sigmoid_gate)))
    grad_up = grad_hidden * active
    grad_pair = jnp.concatenate(
        [grad_gate.astype(jnp.bfloat16), grad_up.astype(jnp.bfloat16)], axis=1
    )
    returned = lax.dot_general(
        grad_pair, pair_weights, (((1,), (1,)), ((), ())), preferred_element_type=jnp.float32
    )
    return (returned.astype(jnp.bfloat16), hidden, grad_pair)


def weight_term(rows_in, grad_in, hidden, grad_pair, grad_scale):
    contract = (((0,), (0,)), ((), ()))
    first_part = lax.dot_general(rows_in, grad_pair, contract, preferred_element_type=jnp.float32)
    second = lax.dot_general(grad_in, hidden, contract, preferred_element_type=jnp.float32)
    return grad_scale * jnp.concatenate([first_part, second], axis=1)


def sum_weights(rows_in, grad_in, hidden, grad_pair, grad_scale):
    term = weight_term(rows_in, grad_in, hidden, grad_pair, grad_scale).astype(jnp.bfloat16)
    bands = term.reshape(lax.axis_size(DP), -1, term.shape[1])
    bands = lax.all_to_all(bands, DP, split_axis=0, concat_axis=0, tiled=True)
    return lax.psum_scatter(bands, "expert", scatter_dimension=0, tiled=False).astype(jnp.float32)


def local(tokens, out_grad, gate_prob, routing, expert_weights):
    tok_dev, model_width = tokens.shape
    experts = lax.axis_size("expert")
    replicas = lax.axis_size(DP)
    capacity = 2 * tok_dev // experts
    share_rows = model_width // replicas
    grad_scale = float(tok_dev * replicas) ** (-0.5)
    width = expert_weights.shape[2]
    band = lax.dynamic_slice_in_dim(
        expert_weights[0], lax.axis_index(DP) * share_rows, share_rows, 0
    )
    bands = lax.all_gather(band, "expert", axis=0, tiled=False)
    scaled = (gate_prob * out_grad.astype(jnp.float32)).astype(jnp.bfloat16)
    slot_index = slot_of(routing[:, 0], capacity, experts)
    dispatch_table = (
        jnp.arange(experts * capacity, dtype=jnp.int32)[:, None] == slot_index[None, :]
    ).astype(jnp.bfloat16)
    send_x = (
        jnp.dot(dispatch_table, tokens, preferred_element_type=jnp.float32)
        .astype(jnp.bfloat16)
        .reshape(experts, capacity, model_width)
    )
    send_g = (
        jnp.dot(dispatch_table, scaled, preferred_element_type=jnp.float32)
        .astype(jnp.bfloat16)
        .reshape(experts, capacity, model_width)
    )
    recv_x, recv_g = side_by_side((send_x, send_g), DP, 0, 0, 1)
    rows_in = recv_x.reshape(experts * capacity, model_width)
    grad_in = recv_g.reshape(experts * capacity, model_width)
    weights = lax.all_to_all(bands, DP, split_axis=0, concat_axis=0, tiled=True)
    weights = weights.reshape(model_width, width)
    returned, hidden, grad_pair = expert_rows(weights, rows_in, grad_in)
    returned = returned.reshape(experts, capacity, model_width)
    summed = sum_weights(rows_in, grad_in, hidden, grad_pair, grad_scale)
    arrived = lax.all_to_all(returned, DP, split_axis=0, concat_axis=0, tiled=True)
    input_grad = lax.dot_general(
        dispatch_table,
        arrived.reshape(experts * capacity, model_width),
        (((0,), (0,)), ((), ())),
        preferred_element_type=jnp.float32,
    ).astype(jnp.bfloat16)
    return (input_grad, summed.reshape(1, share_rows, width))


def solution(mesh):
    split = Mesh(
        mesh.devices.reshape(4, 4, 2, mesh.shape["expert"]), ("dp_0", "dp_1", "dp_2", "expert")
    )
    placed = (
        P(DP_EXPERT, None),
        P(DP_EXPERT, None),
        P(DP_EXPERT, None),
        P(DP_EXPERT, None),
        P("expert", None, None),
    )
    return jax.shard_map(
        local,
        mesh=split,
        in_specs=placed,
        out_specs=(P(DP_EXPERT, None), P("expert", DP, None)),
        check_vma=False,
    )
```

```python
import functools

import jax
import jax.numpy as jnp
from jax import lax
from jax.experimental import pallas as pl
from jax.experimental.pallas import tpu as pltpu
from jax.sharding import PartitionSpec as P

MESH = pl.DeviceIdType.MESH
CHUNKS = 64


def place(n, planes):
    mine = lax.axis_index("dp")
    plane = lax.axis_index("expert")
    expert = mine // 2 + (n // 2) * (mine % 2)
    return plane, mine, (plane - expert + planes) % planes


def meet(n, planes, plane, mine):
    barrier = pltpu.get_barrier_semaphore()

    @pl.loop(1, n)
    def _(k):
        pl.semaphore_signal(
            barrier, inc=1, device_id=((mine + k) % n, plane), device_id_type=MESH
        )

    for step in (1, planes - 1):
        pl.semaphore_signal(
            barrier, inc=1, device_id=(mine, (plane + step) % planes), device_id_type=MESH
        )
    pl.semaphore_wait(barrier, n + 1)


def exchange(n, plane, mine, source, target, send_sem, recv_sem):
    def copy(k):
        peer = (mine + k) % n
        return pltpu.make_async_remote_copy(
            src_ref=source.at[peer],
            dst_ref=target.at[mine],
            send_sem=send_sem.at[k],
            recv_sem=recv_sem.at[k],
            device_id=(peer, plane),
            device_id_type=MESH,
        )

    return copy, pltpu.make_async_copy(source.at[mine], target.at[mine], recv_sem.at[0])


def gather_kernel(n, planes, own_ref, rows_ref, weights_ref, recv_ref, w_send, w_down, w_recv, t_send, t_recv):
    plane, mine, far = place(n, planes)
    half = planes // 2
    origin = far == 0
    onward = jnp.logical_and(far != half, far != half + 1)
    step = jnp.where(far <= half, 1, planes - 1)
    depth = weights_ref.shape[0] // CHUNKS

    def chunk(k):
        return pl.ds(pl.multiple_of(k * depth, depth), depth)

    def local(k):
        return pltpu.make_async_copy(own_ref.at[chunk(k)], weights_ref.at[chunk(k)], w_recv.at[k])

    def hop(k, by, sem):
        return pltpu.make_async_remote_copy(
            src_ref=weights_ref.at[chunk(k)],
            dst_ref=weights_ref.at[chunk(k)],
            send_sem=sem.at[k],
            recv_sem=w_recv.at[k],
            device_id=(mine, (plane + by) % planes),
            device_id_type=MESH,
        )

    @pl.when(origin)
    def _():
        @pl.loop(0, CHUNKS)
        def _(k):
            local(k).start()

    meet(n, planes, plane, mine)
    copy, stay = exchange(n, plane, mine, rows_ref, recv_ref, t_send, t_recv)
    stay.start()

    @pl.loop(1, n)
    def _(k):
        copy(k).start()

    @pl.loop(0, CHUNKS)
    def _(k):
        local(k).wait()

        @pl.when(onward)
        def _():
            hop(k, step, w_send).start()

        @pl.when(origin)
        def _():
            hop(k, planes - 1, w_down).start()

    stay.wait()

    @pl.loop(1, n)
    def _(k):
        copy(k).wait()

    @pl.when(onward)
    def _():
        @pl.loop(0, CHUNKS)
        def _(k):
            hop(k, step, w_send).wait_send()

    @pl.when(origin)
    def _():
        @pl.loop(0, CHUNKS)
        def _(k):
            hop(k, planes - 1, w_down).wait_send()


def reduce_kernel(
    n, planes, part_ref, back_ref, band_ref, recv_ref, inbox, total, c_send, c_recv, b_send, b_recv, t_send, t_recv
):
    plane, mine, far = place(n, planes)
    half = planes // 2
    origin = far == 0
    first = jnp.logical_or(far == half, far == half + 1)
    middle = jnp.logical_not(jnp.logical_or(origin, first))
    step = jnp.where(far <= half, planes - 1, 1)
    side = jnp.where(far == planes - 1, 1, 0)
    depth = part_ref.shape[0] // CHUNKS
    pieces = band_ref.shape[0] // depth

    def chunk(k):
        return pl.ds(pl.multiple_of(k * depth, depth), depth)

    def hop(k, to, source):
        return pltpu.make_async_remote_copy(
            src_ref=source.at[chunk(k)],
            dst_ref=inbox.at[to, chunk(k)],
            send_sem=c_send.at[k],
            recv_sem=c_recv.at[to, k],
            device_id=(mine, (plane + step) % planes),
            device_id_type=MESH,
        )

    def spread(k):
        return pltpu.make_async_remote_copy(
            src_ref=total.at[chunk(k)],
            dst_ref=band_ref.at[chunk(k % pieces)],
            send_sem=b_send.at[k],
            recv_sem=b_recv.at[k % pieces],
            device_id=(k // pieces, plane),
            device_id_type=MESH,
        )

    def keep(k):
        return pltpu.make_async_copy(
            total.at[chunk(k)], band_ref.at[chunk(k % pieces)], b_recv.at[k % pieces]
        )

    meet(n, planes, plane, mine)

    @pl.when(first)
    def _():
        @pl.loop(0, CHUNKS)
        def _(k):
            hop(k, side, part_ref).start()

    copy, stay = exchange(n, plane, mine, back_ref, recv_ref, t_send, t_recv)
    stay.start()

    @pl.loop(1, n)
    def _(k):
        copy(k).start()

    @pl.when(middle)
    def _():
        @pl.loop(0, CHUNKS)
        def _(k):
            hop(k, 0, total).wait_recv()
            rows = chunk(k)
            total[rows, :] = (
                inbox[0, rows, :].astype(jnp.float32) + part_ref[rows, :].astype(jnp.float32)
            ).astype(jnp.bfloat16)
            hop(k, side, total).start()

    @pl.when(origin)
    def _():
        @pl.loop(0, CHUNKS)
        def _(k):
            hop(k, 0, total).wait_recv()
            hop(k, 1, total).wait_recv()
            rows = chunk(k)
            total[rows, :] = (
                inbox[0, rows, :].astype(jnp.float32)
                + inbox[1, rows, :].astype(jnp.float32)
                + part_ref[rows, :].astype(jnp.float32)
            ).astype(jnp.bfloat16)

            @pl.when(k // pieces != mine)
            def _():
                spread(k).start()

            @pl.when(k // pieces == mine)
            def _():
                keep(k).start()

    stay.wait()

    @pl.loop(1, n)
    def _(k):
        copy(k).wait()

    @pl.when(jnp.logical_not(origin))
    def _():
        @pl.loop(0, CHUNKS)
        def _(k):
            hop(k, side, total).wait_send()

    @pl.when(origin)
    def _():
        @pl.loop(0, CHUNKS)
        def _(k):
            @pl.when(k // pieces != mine)
            def _():
                spread(k).wait_send()

    @pl.loop(0, pieces)
    def _(k):
        keep(k).wait()


def slot_of(route_block, capacity, experts):
    onehot = (route_block[:, None] == jnp.arange(experts, dtype=jnp.int32)[None, :]).astype(
        jnp.int32
    )
    before = jnp.cumsum(onehot, axis=0) - onehot
    position = jnp.sum(before * onehot, axis=1)
    holder = 2 * (route_block % (experts // 2)) + route_block // (experts // 2)
    return holder * capacity + position


def expert_rows(weights, rows_in, grad_in):
    hidden_width = weights.shape[1] // 3
    pair_weights = weights[:, : 2 * hidden_width]
    down_weights = weights[:, 2 * hidden_width :]
    pre_act = jnp.dot(rows_in, pair_weights, preferred_element_type=jnp.float32)
    pre_gate = pre_act[:, :hidden_width]
    pre_up = pre_act[:, hidden_width:]
    sigmoid_gate = jax.nn.sigmoid(pre_gate)
    active = pre_gate * sigmoid_gate
    hidden = (active * pre_up).astype(jnp.bfloat16)
    grad_hidden = jnp.dot(grad_in, down_weights, preferred_element_type=jnp.float32)
    grad_gate = grad_hidden * pre_up * (sigmoid_gate * (1.0 + pre_gate * (1.0 - sigmoid_gate)))
    grad_up = grad_hidden * active
    grad_pair = jnp.concatenate(
        [grad_gate.astype(jnp.bfloat16), grad_up.astype(jnp.bfloat16)], axis=1
    )
    returned = lax.dot_general(
        grad_pair, pair_weights, (((1,), (1,)), ((), ())), preferred_element_type=jnp.float32
    )
    return (returned.astype(jnp.bfloat16), hidden, grad_pair)


def weight_term(rows_in, grad_in, hidden, grad_pair, grad_scale):
    contract = (((0,), (0,)), ((), ()))
    first_part = lax.dot_general(rows_in, grad_pair, contract, preferred_element_type=jnp.float32)
    second = lax.dot_general(grad_in, hidden, contract, preferred_element_type=jnp.float32)
    return grad_scale * jnp.concatenate([first_part, second], axis=1)


def local(tokens, out_grad, gate_prob, routing, expert_weights):
    tok_dev, model_width = tokens.shape
    planes = lax.axis_size("expert")
    n = lax.axis_size("dp")
    capacity = 2 * tok_dev // planes
    share_rows = model_width // n
    grad_scale = float(tok_dev * n) ** (-0.5)
    width = expert_weights.shape[2]
    vmem = pl.BlockSpec(memory_space=pltpu.VMEM)
    dma = pltpu.SemaphoreType.DMA
    scaled = (gate_prob * out_grad.astype(jnp.float32)).astype(jnp.bfloat16)
    slot_index = slot_of(routing[:, 0], capacity, planes)
    dispatch_table = (
        jnp.arange(planes * capacity, dtype=jnp.int32)[:, None] == slot_index[None, :]
    ).astype(jnp.bfloat16)

    def spread_out(rows):
        return (
            jnp.dot(dispatch_table, rows, preferred_element_type=jnp.float32)
            .astype(jnp.bfloat16)
            .reshape(n, capacity, model_width)
        )

    send = jnp.concatenate([spread_out(tokens), spread_out(scaled)], axis=1)
    weights, received = pl.pallas_call(
        functools.partial(gather_kernel, n, planes),
        out_shape=(
            jax.ShapeDtypeStruct((model_width, width), jnp.bfloat16),
            jax.ShapeDtypeStruct(send.shape, jnp.bfloat16),
        ),
        in_specs=[pl.BlockSpec(memory_space=pl.ANY), vmem],
        out_specs=(vmem, vmem),
        scratch_shapes=[dma((CHUNKS,)), dma((CHUNKS,)), dma((CHUNKS,)), dma((n,)), dma((n,))],
        compiler_params=pltpu.CompilerParams(collective_id=0, has_side_effects=True),
    )(expert_weights[0], send)
    rows_in = received[:, :capacity].reshape(n * capacity, model_width)
    grad_in = received[:, capacity:].reshape(n * capacity, model_width)
    returned, hidden, grad_pair = expert_rows(weights, rows_in, grad_in)
    returned = returned.reshape(n, capacity, model_width)
    term = weight_term(rows_in, grad_in, hidden, grad_pair, grad_scale).astype(jnp.bfloat16)
    band, arrived = pl.pallas_call(
        functools.partial(reduce_kernel, n, planes),
        out_shape=(
            jax.ShapeDtypeStruct((share_rows, width), jnp.bfloat16),
            jax.ShapeDtypeStruct(returned.shape, jnp.bfloat16),
        ),
        in_specs=[vmem, vmem],
        out_specs=(vmem, vmem),
        scratch_shapes=[
            pltpu.VMEM((2, model_width, width), jnp.bfloat16),
            pltpu.VMEM((model_width, width), jnp.bfloat16),
            dma((CHUNKS,)),
            dma((2, CHUNKS)),
            dma((CHUNKS,)),
            dma((CHUNKS // n,)),
            dma((n,)),
            dma((n,)),
        ],
        compiler_params=pltpu.CompilerParams(collective_id=1, has_side_effects=True),
    )(term, returned)
    input_grad = lax.dot_general(
        dispatch_table,
        arrived.reshape(n * capacity, model_width),
        (((0,), (0,)), ((), ())),
        preferred_element_type=jnp.float32,
    ).astype(jnp.bfloat16)
    return (input_grad, band.astype(jnp.float32).reshape(1, share_rows, width))


def solution(mesh):
    both = P(("dp", "expert"), None)
    return jax.shard_map(
        local,
        mesh=mesh,
        in_specs=(both, both, both, both, P("expert", None, None)),
        out_specs=(both, P("expert", "dp", None)),
        check_vma=False,
    )
```

```python
import functools

import jax
import jax.numpy as jnp
from jax import lax
from jax.experimental import pallas as pl
from jax.experimental.pallas import tpu as pltpu
from jax.sharding import PartitionSpec as P

MESH = pl.DeviceIdType.MESH
CHUNKS = 128
TILES = 4
KERNEL_MIB = 48


def place(n, planes):
    mine = lax.axis_index("dp")
    plane = lax.axis_index("expert")
    expert = mine // 2 + (n // 2) * (mine % 2)
    return plane, mine, (plane - expert + planes) % planes


def meet(n, planes, plane, mine):
    barrier = pltpu.get_barrier_semaphore()

    @pl.loop(1, n)
    def _(k):
        pl.semaphore_signal(
            barrier, inc=1, device_id=((mine + k) % n, plane), device_id_type=MESH
        )

    for step in (1, planes - 1):
        pl.semaphore_signal(
            barrier, inc=1, device_id=(mine, (plane + step) % planes), device_id_type=MESH
        )
    pl.semaphore_wait(barrier, n + 1)


def exchange(n, plane, mine, source, target, send_sem, recv_sem):
    rows = source.shape[0] // n

    def block(k):
        return pl.ds(pl.multiple_of(k * rows, rows), rows)

    def copy(k):
        peer = (mine + k) % n
        return pltpu.make_async_remote_copy(
            src_ref=source.at[block(peer)],
            dst_ref=target.at[block(mine)],
            send_sem=send_sem.at[k],
            recv_sem=recv_sem.at[k],
            device_id=(peer, plane),
            device_id_type=MESH,
        )

    stay = pltpu.make_async_copy(source.at[block(mine)], target.at[block(mine)], recv_sem.at[0])
    return copy, stay


def hidden_grads(weights_ref, x_ref, g_ref):
    depth, width = weights_ref.shape
    unit, tile = width // 3, depth // TILES
    pair = 2 * unit
    pre = grad_hidden = None
    for t in range(TILES):
        rows = slice(t * tile, (t + 1) * tile)
        one = jnp.dot(x_ref[:, rows], weights_ref[rows, :pair], preferred_element_type=jnp.float32)
        two = jnp.dot(g_ref[:, rows], weights_ref[rows, pair:], preferred_element_type=jnp.float32)
        pre = one if pre is None else pre + one
        grad_hidden = two if grad_hidden is None else grad_hidden + two
    pre_gate, pre_up = pre[:, :unit], pre[:, unit:]
    sigmoid_gate = jax.nn.sigmoid(pre_gate)
    active = pre_gate * sigmoid_gate
    hidden = (active * pre_up).astype(jnp.bfloat16)
    grad_gate = grad_hidden * pre_up * (sigmoid_gate * (1.0 + pre_gate * (1.0 - sigmoid_gate)))
    grad_up = grad_hidden * active
    grad_pair = jnp.concatenate(
        [grad_gate.astype(jnp.bfloat16), grad_up.astype(jnp.bfloat16)], axis=1
    )
    return hidden, grad_pair


def expert_kernel(
    n, planes, grad_scale, own_ref, x_ref, g_ref, band_ref, arrived_ref,
    weights, x_in, g_in, part, back, inbox, total,
    w_send, w_down, w_recv, c_send, c_recv, b_send, b_recv, t_send, t_recv,
):
    plane, mine, far = place(n, planes)
    half = planes // 2
    origin = far == 0
    end = jnp.logical_or(far == half, far == half + 1)
    up = jnp.where(far <= half, 1, planes - 1)
    home = jnp.where(far <= half, planes - 1, 1)
    side = jnp.where(far == planes - 1, 1, 0)
    depth = weights.shape[0] // CHUNKS
    tile = weights.shape[0] // TILES
    pair = 2 * weights.shape[1] // 3
    pieces = band_ref.shape[0] // depth

    def chunk(k):
        return pl.ds(pl.multiple_of(k * depth, depth), depth)

    def local(k):
        return pltpu.make_async_copy(own_ref.at[chunk(k)], weights.at[chunk(k)], w_recv.at[k])

    def out(k, by, sem):
        return pltpu.make_async_remote_copy(
            src_ref=weights.at[chunk(k)],
            dst_ref=weights.at[chunk(k)],
            send_sem=sem.at[k],
            recv_sem=w_recv.at[k],
            device_id=(mine, (plane + by) % planes),
            device_id_type=MESH,
        )

    def hop(k, to, source):
        return pltpu.make_async_remote_copy(
            src_ref=source.at[chunk(k)],
            dst_ref=inbox.at[to, chunk(k)],
            send_sem=c_send.at[k],
            recv_sem=c_recv.at[to, k],
            device_id=(mine, (plane + home) % planes),
            device_id_type=MESH,
        )

    def spread(k):
        return pltpu.make_async_remote_copy(
            src_ref=total.at[chunk(k)],
            dst_ref=band_ref.at[chunk(k % pieces)],
            send_sem=b_send.at[k],
            recv_sem=b_recv.at[k % pieces],
            device_id=(k // pieces, plane),
            device_id_type=MESH,
        )

    def keep(k):
        return pltpu.make_async_copy(
            total.at[chunk(k)], band_ref.at[chunk(k % pieces)], b_recv.at[k % pieces]
        )

    @pl.when(origin)
    def _():
        @pl.loop(0, CHUNKS)
        def _(k):
            local(k).start()

    meet(n, planes, plane, mine)
    swaps = [
        exchange(n, plane, mine, source, target, t_send.at[c], t_recv.at[c])
        for c, (source, target) in enumerate(((x_ref, x_in), (g_ref, g_in), (back, arrived_ref)))
    ]

    def begin(copy, stay):
        stay.start()

        @pl.loop(1, n)
        def _(k):
            copy(k).start()

    def finish(copy, stay):
        stay.wait()

        @pl.loop(1, n)
        def _(k):
            copy(k).wait()

    begin(*swaps[0])
    begin(*swaps[1])

    @pl.loop(0, CHUNKS)
    def _(k):
        local(k).wait()

        @pl.when(jnp.logical_not(end))
        def _():
            out(k, up, w_send).start()

        @pl.when(origin)
        def _():
            out(k, planes - 1, w_down).start()

    finish(*swaps[0])
    finish(*swaps[1])
    hidden, grad_pair = hidden_grads(weights, x_in, g_in)
    over_rows = (((0,), (0,)), ((), ()))
    for t in range(TILES):
        rows = slice(t * tile, (t + 1) * tile)
        part[rows, :pair] = (
            grad_scale
            * lax.dot_general(x_in[:, rows], grad_pair, over_rows, preferred_element_type=jnp.float32)
        ).astype(jnp.bfloat16)
        part[rows, pair:] = (
            grad_scale
            * lax.dot_general(g_in[:, rows], hidden, over_rows, preferred_element_type=jnp.float32)
        ).astype(jnp.bfloat16)

        @pl.when(end)
        def _():
            @pl.loop(t * CHUNKS // TILES, (t + 1) * CHUNKS // TILES)
            def _(k):
                hop(k, side, part).start()

    for t in range(TILES):
        rows = slice(t * tile, (t + 1) * tile)
        back[:, rows] = lax.dot_general(
            grad_pair,
            weights[rows, :pair],
            (((1,), (1,)), ((), ())),
            preferred_element_type=jnp.float32,
        ).astype(jnp.bfloat16)
    begin(*swaps[2])

    @pl.when(jnp.logical_not(jnp.logical_or(origin, end)))
    def _():
        @pl.loop(0, CHUNKS)
        def _(k):
            hop(k, 0, total).wait_recv()
            rows = chunk(k)
            total[rows, :] = (
                inbox[0, rows, :].astype(jnp.float32) + part[rows, :].astype(jnp.float32)
            ).astype(jnp.bfloat16)
            hop(k, side, total).start()

    @pl.when(origin)
    def _():
        @pl.loop(0, CHUNKS)
        def _(k):
            hop(k, 0, total).wait_recv()
            hop(k, 1, total).wait_recv()
            rows = chunk(k)
            total[rows, :] = (
                inbox[0, rows, :].astype(jnp.float32)
                + inbox[1, rows, :].astype(jnp.float32)
                + part[rows, :].astype(jnp.float32)
            ).astype(jnp.bfloat16)

            @pl.when(k // pieces != mine)
            def _():
                spread(k).start()

            @pl.when(k // pieces == mine)
            def _():
                keep(k).start()

    finish(*swaps[2])

    @pl.when(jnp.logical_not(end))
    def _():
        @pl.loop(0, CHUNKS)
        def _(k):
            out(k, up, w_send).wait_send()

    @pl.when(jnp.logical_not(origin))
    def _():
        @pl.loop(0, CHUNKS)
        def _(k):
            hop(k, side, total).wait_send()

    @pl.when(origin)
    def _():
        @pl.loop(0, CHUNKS)
        def _(k):
            out(k, planes - 1, w_down).wait_send()

            @pl.when(k // pieces != mine)
            def _():
                spread(k).wait_send()

    @pl.loop(0, pieces)
    def _(k):
        keep(k).wait()


def slot_of(route_block, capacity, experts):
    onehot = (route_block[:, None] == jnp.arange(experts, dtype=jnp.int32)[None, :]).astype(
        jnp.int32
    )
    before = jnp.cumsum(onehot, axis=0) - onehot
    position = jnp.sum(before * onehot, axis=1)
    holder = 2 * (route_block % (experts // 2)) + route_block // (experts // 2)
    return holder * capacity + position


def local(tokens, out_grad, gate_prob, routing, expert_weights):
    tok_dev, model_width = tokens.shape
    planes = lax.axis_size("expert")
    n = lax.axis_size("dp")
    capacity = 2 * tok_dev // planes
    share_rows = model_width // n
    grad_scale = float(tok_dev * n) ** (-0.5)
    width = expert_weights.shape[2]
    vmem = pl.BlockSpec(memory_space=pltpu.VMEM)
    dma = pltpu.SemaphoreType.DMA
    scaled = (gate_prob * out_grad.astype(jnp.float32)).astype(jnp.bfloat16)
    slot_index = slot_of(routing[:, 0], capacity, planes)
    dispatch_table = (
        jnp.arange(planes * capacity, dtype=jnp.int32)[:, None] == slot_index[None, :]
    ).astype(jnp.bfloat16)

    def spread_out(rows):
        spread = jnp.dot(dispatch_table, rows, preferred_element_type=jnp.float32)
        return spread.astype(jnp.bfloat16)

    send_x, send_g = spread_out(tokens), spread_out(scaled)
    band, arrived = pl.pallas_call(
        functools.partial(expert_kernel, n, planes, grad_scale),
        out_shape=(
            jax.ShapeDtypeStruct((share_rows, width), jnp.bfloat16),
            jax.ShapeDtypeStruct(send_x.shape, jnp.bfloat16),
        ),
        in_specs=[pl.BlockSpec(memory_space=pl.ANY), vmem, vmem],
        out_specs=(vmem, vmem),
        scratch_shapes=[
            pltpu.VMEM((model_width, width), jnp.bfloat16),
            pltpu.VMEM(send_x.shape, jnp.bfloat16),
            pltpu.VMEM(send_x.shape, jnp.bfloat16),
            pltpu.VMEM((model_width, width), jnp.bfloat16),
            pltpu.VMEM(send_x.shape, jnp.bfloat16),
            pltpu.VMEM((2, model_width, width), jnp.bfloat16),
            pltpu.VMEM((model_width, width), jnp.bfloat16),
            dma((CHUNKS,)),
            dma((CHUNKS,)),
            dma((CHUNKS,)),
            dma((CHUNKS,)),
            dma((2, CHUNKS)),
            dma((CHUNKS,)),
            dma((CHUNKS // n,)),
            dma((3, n)),
            dma((3, n)),
        ],
        compiler_params=pltpu.CompilerParams(
            collective_id=0, has_side_effects=True, vmem_limit_bytes=KERNEL_MIB << 20
        ),
    )(expert_weights[0], send_x, send_g)
    input_grad = lax.dot_general(
        dispatch_table,
        arrived,
        (((0,), (0,)), ((), ())),
        preferred_element_type=jnp.float32,
    ).astype(jnp.bfloat16)
    return (input_grad, band.astype(jnp.float32).reshape(1, share_rows, width))


def solution(mesh):
    both = P(("dp", "expert"), None)
    return jax.shard_map(
        local,
        mesh=mesh,
        in_specs=(both, both, both, both, P("expert", None, None)),
        out_specs=(both, P("expert", "dp", None)),
        check_vma=False,
    )
```

```python
import functools

import jax
import jax.numpy as jnp
from jax import lax
from jax.experimental import pallas as pl
from jax.experimental.pallas import tpu as pltpu
from jax.sharding import PartitionSpec as P

MESH = pl.DeviceIdType.MESH
CHUNKS = 128
TILES = 4
KERNEL_MIB = 48


def place(n, planes):
    mine = lax.axis_index("dp")
    plane = lax.axis_index("expert")
    expert = mine // 2 + (n // 2) * (mine % 2)
    return plane, mine, (plane - expert + planes) % planes


def meet(n, planes, plane, mine):
    barrier = pltpu.get_barrier_semaphore()

    @pl.loop(1, n)
    def _(k):
        pl.semaphore_signal(
            barrier, inc=1, device_id=((mine + k) % n, plane), device_id_type=MESH
        )

    for step in (1, planes - 1):
        pl.semaphore_signal(
            barrier, inc=1, device_id=(mine, (plane + step) % planes), device_id_type=MESH
        )
    pl.semaphore_wait(barrier, n + 1)


def exchange(n, plane, mine, source, target, send_sem, recv_sem):
    rows = source.shape[0] // n

    def block(k):
        return pl.ds(pl.multiple_of(k * rows, rows), rows)

    def copy(k):
        peer = (mine + k) % n
        return pltpu.make_async_remote_copy(
            src_ref=source.at[block(peer)],
            dst_ref=target.at[block(mine)],
            send_sem=send_sem.at[k],
            recv_sem=recv_sem.at[k],
            device_id=(peer, plane),
            device_id_type=MESH,
        )

    stay = pltpu.make_async_copy(source.at[block(mine)], target.at[block(mine)], recv_sem.at[0])
    return copy, stay


def hidden_grads(weights_ref, x_ref, g_ref):
    depth, width = weights_ref.shape
    unit, tile = width // 3, depth // TILES
    pair = 2 * unit
    pre = grad_hidden = None
    for t in range(TILES):
        rows = slice(t * tile, (t + 1) * tile)
        one = jnp.dot(x_ref[:, rows], weights_ref[rows, :pair], preferred_element_type=jnp.float32)
        two = jnp.dot(g_ref[:, rows], weights_ref[rows, pair:], preferred_element_type=jnp.float32)
        pre = one if pre is None else pre + one
        grad_hidden = two if grad_hidden is None else grad_hidden + two
    pre_gate, pre_up = pre[:, :unit], pre[:, unit:]
    sigmoid_gate = jax.nn.sigmoid(pre_gate)
    active = pre_gate * sigmoid_gate
    hidden = (active * pre_up).astype(jnp.bfloat16)
    grad_gate = grad_hidden * pre_up * (sigmoid_gate * (1.0 + pre_gate * (1.0 - sigmoid_gate)))
    grad_up = grad_hidden * active
    grad_pair = jnp.concatenate(
        [grad_gate.astype(jnp.bfloat16), grad_up.astype(jnp.bfloat16)], axis=1
    )
    return hidden, grad_pair


def expert_kernel(
    n, planes, grad_scale, own_ref, x_ref, g_ref, band_ref, arrived_ref,
    weights, x_in, g_in, part, back, inbox, total,
    w_send, w_down, w_recv, c_send, c_recv, b_send, b_recv, t_send, t_recv,
):
    plane, mine, far = place(n, planes)
    half = planes // 2
    origin = far == 0
    end = jnp.logical_or(far == half, far == half + 1)
    up = jnp.where(far <= half, 1, planes - 1)
    home = jnp.where(far <= half, planes - 1, 1)
    side = jnp.where(far == planes - 1, 1, 0)
    depth = weights.shape[0] // CHUNKS
    tile = weights.shape[0] // TILES
    pair = 2 * weights.shape[1] // 3
    pieces = band_ref.shape[0] // depth

    def chunk(k):
        return pl.ds(pl.multiple_of(k * depth, depth), depth)

    def local(k):
        return pltpu.make_async_copy(own_ref.at[chunk(k)], weights.at[chunk(k)], w_recv.at[k])

    def out(k, by, sem):
        return pltpu.make_async_remote_copy(
            src_ref=weights.at[chunk(k)],
            dst_ref=weights.at[chunk(k)],
            send_sem=sem.at[k],
            recv_sem=w_recv.at[k],
            device_id=(mine, (plane + by) % planes),
            device_id_type=MESH,
        )

    def hop(k, to, source):
        return pltpu.make_async_remote_copy(
            src_ref=source.at[chunk(k)],
            dst_ref=inbox.at[to, chunk(k)],
            send_sem=c_send.at[k],
            recv_sem=c_recv.at[to, k],
            device_id=(mine, (plane + home) % planes),
            device_id_type=MESH,
        )

    def spread(k):
        return pltpu.make_async_remote_copy(
            src_ref=total.at[chunk(k)],
            dst_ref=band_ref.at[chunk(k % pieces)],
            send_sem=b_send.at[k],
            recv_sem=b_recv.at[k % pieces],
            device_id=(k // pieces, plane),
            device_id_type=MESH,
        )

    def keep(k):
        return pltpu.make_async_copy(
            total.at[chunk(k)], band_ref.at[chunk(k % pieces)], b_recv.at[k % pieces]
        )

    @pl.when(origin)
    def _():
        @pl.loop(0, CHUNKS)
        def _(k):
            local(k).start()

    meet(n, planes, plane, mine)
    swaps = [
        exchange(n, plane, mine, source, target, t_send.at[c], t_recv.at[c])
        for c, (source, target) in enumerate(((x_ref, x_in), (g_ref, g_in), (back, arrived_ref)))
    ]

    def begin(copy, stay):
        stay.start()

        @pl.loop(1, n)
        def _(k):
            copy(k).start()

    def finish(copy, stay):
        stay.wait()

        @pl.loop(1, n)
        def _(k):
            copy(k).wait()

    def pass_on(k):
        local(k).wait()

        @pl.when(jnp.logical_not(end))
        def _():
            out(k, up, w_send).start()

        @pl.when(origin)
        def _():
            out(k, planes - 1, w_down).start()

    ahead = jnp.where(origin, CHUNKS // 4, 0)
    pl.loop(0, ahead)(pass_on)
    begin(*swaps[0])
    begin(*swaps[1])
    pl.loop(ahead, CHUNKS)(pass_on)
    finish(*swaps[0])
    finish(*swaps[1])
    hidden, grad_pair = hidden_grads(weights, x_in, g_in)
    over_rows = (((0,), (0,)), ((), ()))
    for t in range(TILES):
        rows = slice(t * tile, (t + 1) * tile)
        part[rows, :pair] = (
            grad_scale
            * lax.dot_general(x_in[:, rows], grad_pair, over_rows, preferred_element_type=jnp.float32)
        ).astype(jnp.bfloat16)
        part[rows, pair:] = (
            grad_scale
            * lax.dot_general(g_in[:, rows], hidden, over_rows, preferred_element_type=jnp.float32)
        ).astype(jnp.bfloat16)

        @pl.when(end)
        def _():
            @pl.loop(t * CHUNKS // TILES, (t + 1) * CHUNKS // TILES)
            def _(k):
                hop(k, side, part).start()

    for t in range(TILES):
        rows = slice(t * tile, (t + 1) * tile)
        back[:, rows] = lax.dot_general(
            grad_pair,
            weights[rows, :pair],
            (((1,), (1,)), ((), ())),
            preferred_element_type=jnp.float32,
        ).astype(jnp.bfloat16)
    begin(*swaps[2])

    @pl.when(jnp.logical_not(jnp.logical_or(origin, end)))
    def _():
        @pl.loop(0, CHUNKS)
        def _(k):
            hop(k, 0, total).wait_recv()
            rows = chunk(k)
            total[rows, :] = (
                inbox[0, rows, :].astype(jnp.float32) + part[rows, :].astype(jnp.float32)
            ).astype(jnp.bfloat16)
            hop(k, side, total).start()

    @pl.when(origin)
    def _():
        @pl.loop(0, CHUNKS)
        def _(k):
            hop(k, 0, total).wait_recv()
            hop(k, 1, total).wait_recv()
            rows = chunk(k)
            total[rows, :] = (
                inbox[0, rows, :].astype(jnp.float32)
                + inbox[1, rows, :].astype(jnp.float32)
                + part[rows, :].astype(jnp.float32)
            ).astype(jnp.bfloat16)

            @pl.when(k // pieces != mine)
            def _():
                spread(k).start()

            @pl.when(k // pieces == mine)
            def _():
                keep(k).start()

    finish(*swaps[2])

    @pl.when(jnp.logical_not(end))
    def _():
        @pl.loop(0, CHUNKS)
        def _(k):
            out(k, up, w_send).wait_send()

    @pl.when(jnp.logical_not(origin))
    def _():
        @pl.loop(0, CHUNKS)
        def _(k):
            hop(k, side, total).wait_send()

    @pl.when(origin)
    def _():
        @pl.loop(0, CHUNKS)
        def _(k):
            out(k, planes - 1, w_down).wait_send()

            @pl.when(k // pieces != mine)
            def _():
                spread(k).wait_send()

    @pl.loop(0, pieces)
    def _(k):
        keep(k).wait()


def slot_of(route_block, capacity, experts):
    order = jnp.arange(route_block.shape[0], dtype=jnp.int32)
    same = route_block[:, None] == route_block[None, :]
    earlier = order[None, :] < order[:, None]
    position = jnp.sum(jnp.logical_and(same, earlier).astype(jnp.int32), axis=1)
    holder = 2 * (route_block % (experts // 2)) + route_block // (experts // 2)
    return holder * capacity + position


def local(tokens, out_grad, gate_prob, routing, expert_weights):
    tok_dev, model_width = tokens.shape
    planes = lax.axis_size("expert")
    n = lax.axis_size("dp")
    capacity = 2 * tok_dev // planes
    share_rows = model_width // n
    grad_scale = float(tok_dev * n) ** (-0.5)
    width = expert_weights.shape[2]
    vmem = pl.BlockSpec(memory_space=pltpu.VMEM)
    dma = pltpu.SemaphoreType.DMA
    scaled = (gate_prob * out_grad.astype(jnp.float32)).astype(jnp.bfloat16)
    slot_index = slot_of(routing[:, 0], capacity, planes)
    dispatch_table = (
        jnp.arange(planes * capacity, dtype=jnp.int32)[:, None] == slot_index[None, :]
    ).astype(jnp.bfloat16)

    def spread_out(rows):
        spread = jnp.dot(dispatch_table, rows, preferred_element_type=jnp.float32)
        return spread.astype(jnp.bfloat16)

    send_x, send_g = spread_out(tokens), spread_out(scaled)
    band, arrived = pl.pallas_call(
        functools.partial(expert_kernel, n, planes, grad_scale),
        out_shape=(
            jax.ShapeDtypeStruct((share_rows, width), jnp.bfloat16),
            jax.ShapeDtypeStruct(send_x.shape, jnp.bfloat16),
        ),
        in_specs=[pl.BlockSpec(memory_space=pl.ANY), vmem, vmem],
        out_specs=(vmem, vmem),
        scratch_shapes=[
            pltpu.VMEM((model_width, width), jnp.bfloat16),
            pltpu.VMEM(send_x.shape, jnp.bfloat16),
            pltpu.VMEM(send_x.shape, jnp.bfloat16),
            pltpu.VMEM((model_width, width), jnp.bfloat16),
            pltpu.VMEM(send_x.shape, jnp.bfloat16),
            pltpu.VMEM((2, model_width, width), jnp.bfloat16),
            pltpu.VMEM((model_width, width), jnp.bfloat16),
            dma((CHUNKS,)),
            dma((CHUNKS,)),
            dma((CHUNKS,)),
            dma((CHUNKS,)),
            dma((2, CHUNKS)),
            dma((CHUNKS,)),
            dma((CHUNKS // n,)),
            dma((3, n)),
            dma((3, n)),
        ],
        compiler_params=pltpu.CompilerParams(
            collective_id=0, has_side_effects=True, vmem_limit_bytes=KERNEL_MIB << 20
        ),
    )(expert_weights[0], send_x, send_g)
    input_grad = lax.dot_general(
        dispatch_table,
        arrived,
        (((0,), (0,)), ((), ())),
        preferred_element_type=jnp.float32,
    ).astype(jnp.bfloat16)
    return (input_grad, band.astype(jnp.float32).reshape(1, share_rows, width))


def solution(mesh):
    both = P(("dp", "expert"), None)
    return jax.shard_map(
        local,
        mesh=mesh,
        in_specs=(both, both, both, both, P("expert", None, None)),
        out_specs=(both, P("expert", "dp", None)),
        check_vma=False,
    )
```
